512 devices in a mesh: seq: 128 (over x, z_hi, y), tp: 4 (over z_lo, core).
Axes of the slice: x: 4, y: 8, z: 8 (z_hi: 4, z_lo: 2; z = z_hi * 2 + z_lo), core: 2. Of those that a mesh axis runs over, the one named last changes fastest.
Arguments:
- queries: bfloat16 [16384, 4096], P('seq', 'tp'), may hold values from -16 to 16
- keyvalues: bfloat16 [2, 16384, 1024], P(None, 'seq', 'tp'), may hold values from -16 to 16
- stretch_order: int32 [128], replicated, may hold values from 0 to 127, each once
- block_table: int32 [128, 128], replicated, may hold values 0 or 1
- proj_weight: bfloat16 [4096, 2048], P('tp'), may hold values from -0.09375 to 0.09375
Outputs:
- projected: bfloat16 [16384, 2048], P('seq', 'tp')
The draws below stay inside these ranges and needn't reach their ends.
Inputs may be any that keep to these rules, and one draw needn't show every extreme that they name: `stretch_order`: every stretch number 0 to 127 appears once. `block_table`: entry [i, j] matters only where j < i.
All inputs are finite; a program needn't handle non-finite values.
Results may differ from the reference program's by a relative error of at most 0.014.
Values may be sent and summed in bfloat16 or wider, within the bound.
No kernel may reach another device: no remote copies, remote signals or barrier semaphores. Data moves between devices by JAX's collectives and lax.ppermute only.
A program may use at most 128 MiB of HBM per device.

```python
import jax
import jax.numpy as jnp
from jax import lax

QUERY_HEADS = 32
KEY_VALUE_HEADS = 8
HEAD_SIZE = 128
DOUT = 2048
STRETCH_TOKENS = 128
NCHUNK = 128
SEQUENCE_TOKENS = 16384


def query_key_pair(key):
    base = jax.random.fold_in(key, 11)
    random_seeds = jax.random.split(base, 3)
    queries = jnp.clip(jax.random.normal(random_seeds[0], (SEQUENCE_TOKENS, QUERY_HEADS * HEAD_SIZE), jnp.float32), -4.0, 4.0)
    key_matrix = jnp.clip(jax.random.normal(random_seeds[1], (SEQUENCE_TOKENS, KEY_VALUE_HEADS * HEAD_SIZE), jnp.float32), -4.0, 4.0)
    value_vectors = jnp.clip(jax.random.normal(random_seeds[2], (SEQUENCE_TOKENS, KEY_VALUE_HEADS * HEAD_SIZE), jnp.float32), -4.0, 4.0)
    return (queries, jnp.stack([key_matrix, value_vectors]))


def draw_queries(key, part):
    return query_key_pair(key)[0].astype(jnp.bfloat16)


def draw_keyvalues(key, part):
    return query_key_pair(key)[1].astype(jnp.bfloat16)


def set_ends(drawn, stream_key, low, top_value):
    longest = drawn.shape.index(max(drawn.shape))
    spots = []
    for shift in (0, 1):
        where = [jax.random.randint(jax.random.fold_in(stream_key, axis), (), 0, length) for axis, length in enumerate(drawn.shape)]
        where[longest] = (where[longest] + shift) % drawn.shape[longest]
        spots.append(tuple(where))
    return drawn.at[spots[0]].set(low).at[spots[1]].set(top_value)


def level_of(key, extent, cuts, low, top_value):
    factor_of = 1.0
    for dim, parts in cuts:
        steps = jax.random.uniform(jax.random.fold_in(jax.random.fold_in(key, 6), dim), (parts,), jnp.float32, low / len(cuts), top_value / len(cuts))
        factor_of = factor_of * jnp.repeat(jnp.exp(steps), extent[dim] // parts).reshape((-1,) + (1,) * (len(extent) - 1 - dim))
    return factor_of


def scatter_about(rng, dims, width, limit, pieces=(), kind=jnp.bfloat16):
    values = jax.random.normal(rng, dims, jnp.float32) * width
    if len(pieces) > 0:
        values = level_of(rng, dims, pieces, -0.22, 0.18) * values
    return jnp.clip(values, min=-limit, max=limit).astype(kind)


def setup_inputs(seed: int = 0) -> dict:
    key_of = jax.random.split(jax.random.key(seed), 6)
    queries = draw_queries(jax.random.fold_in(key_of[5], 71), 0)
    keyvalues = draw_keyvalues(jax.random.fold_in(key_of[5], 71), 0)
    stretch_order = jax.random.permutation(key_of[2], NCHUNK).astype(jnp.int32)
    block_table = set_ends((jax.random.randint(key_of[3], (NCHUNK, NCHUNK), 0, 4) < 3).astype(jnp.int32), jax.random.fold_in(key_of[3], 1), 0, 1)
    proj_weight = scatter_about(key_of[4], (QUERY_HEADS * HEAD_SIZE, DOUT), (QUERY_HEADS * HEAD_SIZE) ** -0.5, 0.09375, ((0, 4),))
    return {"queries": queries, "keyvalues": keyvalues, "stretch_order": stretch_order, "block_table": block_table, "proj_weight": proj_weight}


def reference(queries, keyvalues, stretch_order, block_table, proj_weight):
    row_index = jnp.arange(SEQUENCE_TOKENS, dtype=jnp.int32)
    row_stretch = stretch_order[row_index // STRETCH_TOKENS].astype(jnp.int32)
    row_pos = row_stretch * STRETCH_TOKENS + row_index % STRETCH_TOKENS
    group_width = QUERY_HEADS // KEY_VALUE_HEADS
    score_scale = 1.0 / (HEAD_SIZE ** 0.5)
    key_matrix = keyvalues[0].astype(jnp.float32).reshape(SEQUENCE_TOKENS, KEY_VALUE_HEADS, HEAD_SIZE)
    value_matrix = keyvalues[1].astype(jnp.float32).reshape(SEQUENCE_TOKENS, KEY_VALUE_HEADS, HEAD_SIZE)

    def block_out(block_index):
        start = (block_index * STRETCH_TOKENS).astype(jnp.int32)
        query_tile = lax.dynamic_slice_in_dim(queries, start, STRETCH_TOKENS, 0).astype(jnp.float32)
        query_tile = query_tile.reshape(STRETCH_TOKENS, KEY_VALUE_HEADS, group_width, HEAD_SIZE)
        query_stretch = lax.dynamic_slice_in_dim(row_stretch, start, STRETCH_TOKENS, 0)
        query_pos = lax.dynamic_slice_in_dim(row_pos, start, STRETCH_TOKENS, 0)
        table_row = block_table[query_stretch[0]]
        table_hits = table_row[row_stretch]
        same_stretch = (row_stretch[None, :] == query_stretch[:, None]) & (row_pos[None, :] <= query_pos[:, None])
        earlier = (row_stretch[None, :] < query_stretch[:, None]) & (table_hits[None, :] == 1)
        allowed = same_stretch | earlier
        scores = jnp.einsum("tkgd,skd->kgts", query_tile, key_matrix) * score_scale
        scores = jnp.where(allowed, scores, -1e30)
        row_max = jnp.max(scores, axis=-1)
        weights = jnp.where(allowed, jnp.exp(scores - row_max[..., None]), 0.0)
        denominator = jnp.sum(weights, axis=-1)
        rounded = weights.astype(jnp.bfloat16).astype(jnp.float32)
        numerator = jnp.einsum("kgts,skd->kgtd", rounded, value_matrix)
        attended = numerator / denominator[..., None]
        attended = jnp.transpose(attended, (2, 0, 1, 3)).reshape(STRETCH_TOKENS, QUERY_HEADS * HEAD_SIZE)
        return attended.astype(jnp.bfloat16)

    blocks = lax.map(block_out, jnp.arange(NCHUNK, dtype=jnp.int32))
    attention = blocks.reshape(SEQUENCE_TOKENS, QUERY_HEADS * HEAD_SIZE)
    return jnp.dot(attention, proj_weight, preferred_element_type=jnp.float32).astype(jnp.bfloat16)
```

```python
import functools

import jax
import jax.numpy as jnp
from jax import lax
from jax.experimental import pallas as pl
from jax.experimental.pallas import tpu as pltpu
from jax.sharding import PartitionSpec as P

HEAD = 128
ROWS = 128
NX, NZ, NY = 4, 4, 8
LOG2E = 1.4426950408889634
SCALE2 = LOG2E / HEAD**0.5
NEG = -1e30


def _place(dx, dz, dy):
    pairs = []
    for x in range(NX):
        for z in range(NZ):
            for y in range(NY):
                src = (x * NZ + z) * NY + y
                dst = (((x + dx) % NX) * NZ + (z + dz) % NZ) * NY + (y + dy) % NY
                pairs.append((src, dst))
    return pairs


def _shift(a, dx=0, dz=0, dy=0):
    return lax.ppermute(a, "seq", _place(dx, dz, dy))


X_GROUPS = [[x * NZ * NY + r for x in range(NX)] for r in range(NZ * NY)]
Z_GROUPS = [[(x * NZ + z) * NY + y for z in range(NZ)] for x in range(NX) for y in range(NY)]


def _swap(a, groups):
    return lax.all_to_all(a, "seq", 0, 0, tiled=True, axis_index_groups=groups)


def _flags_kernel(at_ref, order_ref, table_ref, out_ref):
    me = at_ref[0]
    x = me // (NZ * NY)
    z = (me // NY) % NZ
    y = me % NY
    for i in range(NX):
        cq = order_ref[(i * NZ + z) * NY + y]

        def each(k, carry):
            d = k // NZ
            zk = k % NZ
            ck = order_ref[(x * NZ + zk) * NY + (y + d) % NY]
            seen = jnp.where((ck < cq) & (table_ref[cq, ck] == 1), 1, 0)
            out_ref[i * 32 + k] = jnp.where(ck == cq, 2, seen)
            return carry

        lax.fori_loop(0, NY * NZ, each, 0)


def _flags(order, table):
    me = lax.axis_index("seq").astype(jnp.int32).reshape(1)
    smem = pl.BlockSpec(memory_space=pltpu.SMEM)
    return pl.pallas_call(
        _flags_kernel,
        in_specs=[smem, smem, smem],
        out_specs=smem,
        out_shape=jax.ShapeDtypeStruct((NX * 32,), jnp.int32),
        name="flags",
    )(me, order, table)


def _attend_kernel(*refs, dists, own, first, last):
    flag_ref, q_ref = refs[0], refs[1]
    kv_refs = refs[2 : 2 + len(dists)]
    rest = refs[2 + len(dists) :]
    if not first:
        state_in, rest = rest[0], rest[1:]
    out_ref, acc_ref, m_ref = rest
    lane = lax.broadcasted_iota(jnp.int32, (1, 4 * ROWS), 1)

    def per_query(i, carry):
        if first:
            acc_ref[...] = jnp.zeros_like(acc_ref)
            m_ref[...] = jnp.full_like(m_ref, NEG)
        else:
            for h in range(8):
                st = state_in[i, h, :, HEAD:]
                acc_ref[h, :, :HEAD] = state_in[i, h, :, :HEAD]
                acc_ref[h, :, HEAD:] = jnp.broadcast_to(st[:, :1], (ROWS, HEAD))
                m_ref[h] = jnp.broadcast_to(st[:, 64:65], (ROWS, HEAD))
        for kv_ref, parts in zip(kv_refs, dists):
            flags = [flag_ref[i * 32 + d * 4 + zk] for d, zk in parts]
            alive = functools.reduce(jnp.maximum, flags)

            @pl.when(alive > 0)
            def _():
                bias = jnp.full((1, 4 * ROWS), NEG, jnp.float32)
                for n, f in enumerate(flags):
                    bias = jnp.where((lane // ROWS == n) & (f > 0), 0.0, bias)
                if own:
                    full = lax.broadcasted_iota(jnp.int32, (ROWS, 4 * ROWS), 1)
                    row = lax.broadcasted_iota(jnp.int32, (ROWS, 4 * ROWS), 0)
                    self_lane = jnp.zeros((1, 4 * ROWS), jnp.bool_)
                    for n, f in enumerate(flags):
                        self_lane = self_lane | ((lane // ROWS == n) & (f == 2))
                    bias = bias + jnp.where(self_lane & (full % ROWS > row), NEG, 0.0)
                    bias = jnp.concatenate([bias] * 4, axis=0)
                for g in range(2):
                    k = kv_ref[:, :ROWS, g * HEAD : (g + 1) * HEAD].reshape(4 * ROWS, HEAD)
                    v = kv_ref[:, ROWS:, g * HEAD : (g + 1) * HEAD].reshape(4 * ROWS, HEAD)
                    v = jnp.concatenate([v, jnp.ones_like(v)], axis=1)
                    q = jnp.concatenate(
                        [q_ref[i, :, (g * 4 + j) * HEAD : (g * 4 + j + 1) * HEAD] for j in range(4)], axis=0
                    )
                    s = lax.dot_general(q, k, (((1,), (1,)), ((), ())), preferred_element_type=jnp.float32)
                    s = s * SCALE2 + bias
                    m_old = m_ref[g * 4 : g * 4 + 4].reshape(4 * ROWS, HEAD)
                    m_new = jnp.maximum(m_old, jnp.max(s, axis=1, keepdims=True))
                    p = jnp.exp2(s - jnp.concatenate([m_new] * 4, axis=1))
                    pv = jnp.dot(p.astype(jnp.bfloat16), v, preferred_element_type=jnp.float32)
                    factor = jnp.exp2(m_old - m_new)
                    acc = acc_ref[g * 4 : g * 4 + 4].reshape(4 * ROWS, 2 * HEAD)
                    acc = acc * jnp.concatenate([factor, factor], axis=1) + pv
                    acc_ref[g * 4 : g * 4 + 4] = acc.reshape(4, ROWS, 2 * HEAD)
                    m_ref[g * 4 : g * 4 + 4] = m_new.reshape(4, ROWS, HEAD)

        col = lax.broadcasted_iota(jnp.int32, (ROWS, HEAD), 1)
        if last:
            ext = jnp.zeros((ROWS, HEAD), jnp.float32)
            for h in range(8):
                total = acc_ref[h, :, HEAD:]
                some = total > 0.0
                safe = jnp.where(some, total, 1.0)
                out_ref[i, :, h * HEAD : (h + 1) * HEAD] = (acc_ref[h, :, :HEAD] / safe).astype(jnp.bfloat16)
                lse = jnp.where(some, m_ref[h] + jnp.log2(safe), NEG)
                ext = jnp.where(col % 8 == h, lse, ext)
            hi = ext.astype(jnp.bfloat16).astype(jnp.float32)
            left = ext - hi
            mid = left.astype(jnp.bfloat16).astype(jnp.float32)
            ext = jnp.where(col < 8, hi, jnp.where(col < 16, mid, left - mid))
            out_ref[i, :, 8 * HEAD :] = ext.astype(jnp.bfloat16)
        else:
            for h in range(8):
                out_ref[i, h, :, :HEAD] = acc_ref[h, :, :HEAD]
                out_ref[i, h, :, HEAD:] = jnp.where(col < 64, acc_ref[h, :, HEAD:], m_ref[h])
        return carry

    lax.fori_loop(0, NX, per_query, 0)


def _attend(flags, q, chunks, dists, state, own, last, name):
    smem = pl.BlockSpec(memory_space=pltpu.SMEM)
    vmem = pl.BlockSpec(memory_space=pltpu.VMEM)
    first = state is None
    args = [flags, q, *chunks] + ([] if first else [state])
    if last:
        out = jax.ShapeDtypeStruct((NX, ROWS, 9 * HEAD), jnp.bfloat16)
    else:
        out = jax.ShapeDtypeStruct((NX, 8, ROWS, 2 * HEAD), jnp.float32)
    units = NX * len(chunks)
    return pl.pallas_call(
        functools.partial(_attend_kernel, dists=dists, own=own, first=first, last=last),
        in_specs=[smem] + [vmem] * (len(args) - 1),
        out_specs=vmem,
        out_shape=out,
        scratch_shapes=[
            pltpu.VMEM((8, ROWS, 2 * HEAD), jnp.float32),
            pltpu.VMEM((8, ROWS, HEAD), jnp.float32),
        ],
        compiler_params=pltpu.CompilerParams(vmem_limit_bytes=40 * 1024 * 1024),
        cost_estimate=pl.CostEstimate(
            flops=units * 8 * ROWS * 4 * ROWS * HEAD * 4, transcendentals=units * 8 * ROWS * 4 * ROWS, bytes_accessed=4 << 20
        ),
        name=name,
    )(*args)


def _project_kernel(part_ref, w_ref, out_ref, att_ref):
    lses = []
    for x in range(NX):
        ext = part_ref[x, :, 8 * HEAD :].astype(jnp.float32)
        lses.append(ext[:, 0:8] + ext[:, 8:16] + ext[:, 16:24])
    top = functools.reduce(jnp.maximum, lses)
    ws = [jnp.exp2(v - top) for v in lses]
    total = functools.reduce(jnp.add, ws)
    ws = [w / total for w in ws]
    for h in range(8):
        mixed = jnp.zeros((ROWS, HEAD), jnp.float32)
        for x in range(NX):
            mixed += ws[x][:, h : h + 1] * part_ref[x, :, h * HEAD : (h + 1) * HEAD].astype(jnp.float32)
        att_ref[:, h * HEAD : (h + 1) * HEAD] = mixed.astype(jnp.bfloat16)
    for n in range(4):
        out_ref[n] = jnp.dot(
            att_ref[...], w_ref[:, n * 512 : (n + 1) * 512], preferred_element_type=jnp.float32
        ).astype(jnp.bfloat16)


def _project(parts, weight):
    vmem = pl.BlockSpec(memory_space=pltpu.VMEM)
    return pl.pallas_call(
        _project_kernel,
        in_specs=[vmem, vmem],
        out_specs=vmem,
        out_shape=jax.ShapeDtypeStruct((4, ROWS, 512), jnp.bfloat16),
        scratch_shapes=[pltpu.VMEM((ROWS, 8 * HEAD), jnp.bfloat16)],
        compiler_params=pltpu.CompilerParams(vmem_limit_bytes=40 * 1024 * 1024),
        cost_estimate=pl.CostEstimate(flops=2 * ROWS * 1024 * 2048, transcendentals=0, bytes_accessed=5 << 20),
        name="project",
    )(parts, weight)


def per_device(queries, keyvalues, stretch_order, block_table, proj_weight):
    kv = keyvalues.reshape(1, 2 * ROWS, 2 * HEAD)
    near = _swap(jnp.broadcast_to(kv, (NZ, 2 * ROWS, 2 * HEAD)), Z_GROUPS)
    q = _swap(jnp.broadcast_to(queries[None], (NX, ROWS, 8 * HEAD)), X_GROUPS)
    flags = _flags(stretch_order, block_table)

    def full(d):
        return [(d % NY, zk) for zk in range(NZ)]

    f1 = _shift(near, dy=1)
    b1 = _shift(near, dy=-1)
    state = _attend(flags, q, [near], [full(0)], None, True, False, "attend0")
    f2 = _shift(f1, dy=1)
    b2 = _shift(b1, dy=-1)
    state = _attend(flags, q, [f1, b1], [full(-1), full(1)], state, False, False, "attend1")
    f3 = _shift(f2, dy=1)
    b3 = _shift(b2, dy=-1)
    state = _attend(flags, q, [f2, b2], [full(-2), full(2)], state, False, False, "attend2")
    f4 = _shift(f3[:2], dy=1)
    b4 = _shift(b3[2:], dy=-1)
    state = _attend(flags, q, [f3, b3], [full(-3), full(3)], state, False, False, "attend3")
    far = jnp.concatenate([f4, b4], axis=0)
    parts = _attend(flags, q, [far], [full(4)], state, False, True, "attend4")
    mine = _swap(parts, X_GROUPS)
    shares = _project(mine, proj_weight)
    got = lax.all_to_all(shares, "tp", 0, 0, tiled=True)
    return jnp.sum(got.astype(jnp.float32), axis=0).astype(jnp.bfloat16)


def solution(mesh):
    in_specs = (P("seq", "tp"), P(None, "seq", "tp"), P(), P(), P("tp", None))
    return jax.shard_map(
        per_device, mesh=mesh, in_specs=in_specs, out_specs=P("seq", "tp"), check_vma=False
    )
```

```python
import functools

import jax
import jax.numpy as jnp
from jax import lax
from jax.experimental import pallas as pl
from jax.experimental.pallas import tpu as pltpu
from jax.sharding import PartitionSpec as P


HEAD = 128
ROWS = 128
NX, NZ, NY = 4, 4, 8
SCALE2 = 1.4426950408889634 / HEAD**0.5
NEG = -1e30
KEYS = 4


SMEM = pl.BlockSpec(memory_space=pltpu.SMEM)
VMEM = pl.BlockSpec(memory_space=pltpu.VMEM)
PARAMS = pltpu.CompilerParams(vmem_limit_bytes=26 * 1024 * 1024)


def _shift(a, dx=0, dz=0, dy=0):
    pairs = []
    for x in range(NX):
        for z in range(NZ):
            for y in range(NY):
                src = (x * NZ + z) * NY + y
                dst = (((x + dx) % NX) * NZ + (z + dz) % NZ) * NY + (y + dy) % NY
                pairs.append((src, dst))
    return lax.ppermute(a, "seq", pairs)


X_GROUPS = [[x * NZ * NY + r for x in range(NX)] for r in range(NZ * NY)]
Z_GROUPS = [[(x * NZ + z) * NY + y for z in range(NZ)] for x in range(NX) for y in range(NY)]


def _swap(a, groups):
    return lax.all_to_all(a, "seq", 0, 0, tiled=True, axis_index_groups=groups)


def _flags_kernel(at_ref, order_ref, table_ref, out_ref):
    me = at_ref[0]
    x = lax.shift_right_logical(me, 5)
    z = lax.shift_right_logical(me, 3) & 3
    y = me & 7
    for j in range(NX):
        cq = order_ref[((x + j) & 3) * 32 + z * 8 + y]
        for n in range(NZ):
            base = x * 32 + n * 8
            for d in range(NY):
                ck = order_ref[base + ((y + d) & 7)]
                seen = jnp.where((ck < cq) & (table_ref[cq, ck] == 1), 1, 0)
                if j == 0 and d == 0:
                    seen = jnp.where(n == z, 2, seen)
                out_ref[j * 32 + d * 4 + n] = seen
    out_ref[128] = x


def _flags(order, table):
    me = lax.axis_index("seq").astype(jnp.int32).reshape(1)
    return pl.pallas_call(
        _flags_kernel,
        in_specs=[SMEM, SMEM, SMEM],
        out_specs=SMEM,
        out_shape=jax.ShapeDtypeStruct((NX * 32 + 1,), jnp.int32),
        name="flags",
    )(me, order, table)


def _unit(q_ref, i, kv_ref, base, bias, acc_ref, m_ref, j):
    scores = []
    for g in range(2):
        q = jnp.concatenate([q_ref[i, :, (g * 4 + h) * HEAD : (g * 4 + h + 1) * HEAD] for h in range(4)], axis=0)
        k = kv_ref[pl.ds(base, KEYS), :ROWS, g * HEAD : (g + 1) * HEAD].reshape(KEYS * ROWS, HEAD)
        scores.append(lax.dot_general(q, k, (((1,), (1,)), ((), ())), preferred_element_type=jnp.float32))
    for g in range(2):
        v = kv_ref[pl.ds(base, KEYS), ROWS:, g * HEAD : (g + 1) * HEAD].reshape(KEYS * ROWS, HEAD)
        v = jnp.concatenate([v, jnp.ones_like(v)], axis=1)
        s = scores[g] * SCALE2 + bias
        heads = slice(g * 4, g * 4 + 4)
        m_old = m_ref[j, heads].reshape(4 * ROWS, HEAD)
        m_new = jnp.maximum(m_old, jnp.max(s, axis=1, keepdims=True))
        p = jnp.exp2(s - jnp.concatenate([m_new] * KEYS, axis=1))
        pv = jnp.dot(p.astype(jnp.bfloat16), v, preferred_element_type=jnp.float32)
        factor = jnp.exp2(m_old - m_new)
        acc = acc_ref[j, heads].reshape(4 * ROWS, 2 * HEAD)
        acc = acc * jnp.concatenate([factor, factor], axis=1) + pv
        acc_ref[j, heads] = acc.reshape(4, ROWS, 2 * HEAD)
        m_ref[j, heads] = m_new.reshape(4, ROWS, HEAD)


def _finish(acc_ref, m_ref, j, out_ref, i):
    col = lax.broadcasted_iota(jnp.int32, (ROWS, HEAD), 1) % 8
    sums = jnp.zeros((ROWS, HEAD), jnp.float32)
    tops = jnp.zeros((ROWS, HEAD), jnp.float32)
    for h in range(8):
        total = acc_ref[j, h, :, HEAD:]
        safe = jnp.where(total > 0.0, total, 1.0)
        out_ref[i, :, h * HEAD : (h + 1) * HEAD] = (acc_ref[j, h, :, :HEAD] / safe).astype(jnp.bfloat16)
        sums = jnp.where(col == h, total, sums)
        tops = jnp.where(col == h, m_ref[j, h], tops)
    some = sums > 0.0
    ext = jnp.where(some, tops + jnp.log2(jnp.where(some, sums, 1.0)), NEG)
    col = lax.broadcasted_iota(jnp.int32, (ROWS, HEAD), 1)
    hi = ext.astype(jnp.bfloat16).astype(jnp.float32)
    left = ext - hi
    mid = left.astype(jnp.bfloat16).astype(jnp.float32)
    ext = jnp.where(col < 8, hi, jnp.where(col < 16, mid, left - mid))
    out_ref[i, :, 8 * HEAD :] = ext.astype(jnp.bfloat16)


def _attend_kernel(*refs, dists, queries, first, last):
    nq, nc = len(queries), len(dists)
    own = queries == (0,)
    flag_ref, q_ref = refs[:2]
    chunk_refs = refs[2 : 2 + nc]
    rest = list(refs[2 + nc :])
    state = [] if first else [rest.pop(0), rest.pop(0)]
    kv_ref = rest.pop()
    if last:
        out_ref = rest.pop(0)
    acc_ref, m_ref = rest
    for c, ref in enumerate(chunk_refs):
        kv_ref[c * NZ : (c + 1) * NZ] = ref[...]
    if first:
        acc_ref[...] = jnp.zeros_like(acc_ref)
        m_ref[...] = jnp.full_like(m_ref, NEG)
    else:
        acc_ref[...] = state[0][...]
        m_ref[...] = state[1][...]
    lane = lax.broadcasted_iota(jnp.int32, (1, KEYS * ROWS), 1) // ROWS
    x = flag_ref[NX * 32]

    def where_q(j):
        return 0 if own else (x + queries[0] + j) & 3

    def run(j, c, masked):
        at = dists[0]
        for k in range(1, nc):
            at = jnp.where(c == k, dists[k], at)
        flags = [flag_ref[(queries[0] + j) * 32 + at * 4 + n] for n in range(KEYS)]

        @pl.when(functools.reduce(jnp.maximum, flags) > 0)
        def _():
            bias = jnp.full((1, KEYS * ROWS), NEG, jnp.float32)
            for n, f in enumerate(flags):
                bias = jnp.where((lane == n) & (f > 0), 0.0, bias)
            if masked:
                same = jnp.zeros((1, KEYS * ROWS), jnp.float32)
                for n, f in enumerate(flags):
                    same = jnp.where((lane == n) & (f == 2), 1.0, same)
                key = lax.broadcasted_iota(jnp.int32, (ROWS, KEYS * ROWS), 1) % ROWS
                row = lax.broadcasted_iota(jnp.int32, (ROWS, KEYS * ROWS), 0)
                bias = bias + jnp.where(key > row, NEG, 0.0) * same
                bias = jnp.concatenate([bias] * 4, axis=0)
            _unit(q_ref, where_q(j), kv_ref, c * NZ, bias, acc_ref, m_ref, j)

    if own:
        run(0, 0, True)

    def each(u, carry):
        if nq == 1:
            run(0, u, False)
        elif nc == 1:
            run(u, 0, False)
        else:
            run(u // nc, u % nc, False)
        return carry

    lax.fori_loop(1 if own else 0, nq * nc, each, 0)
    if last:
        for j in range(nq):
            _finish(acc_ref, m_ref, j, out_ref, where_q(j))


def _attend(flags, q, chunks, dists, state, last, queries):
    nq, nc = len(queries), len(chunks)
    first = state is None
    args = [flags, q, *chunks] + ([] if first else list(state))
    acc = jax.ShapeDtypeStruct((nq, 8, ROWS, 2 * HEAD), jnp.float32)
    top = jax.ShapeDtypeStruct((nq, 8, ROWS, HEAD), jnp.float32)
    scratch = [pltpu.VMEM((nc * NZ, 2 * ROWS, 2 * HEAD), jnp.bfloat16)]
    if last:
        out = (jax.ShapeDtypeStruct((q.shape[0], ROWS, 9 * HEAD), jnp.bfloat16),)
        scratch = [pltpu.VMEM(acc.shape, acc.dtype), pltpu.VMEM(top.shape, top.dtype)] + scratch
    else:
        out = (acc, top)
    pairs = nq * nc * NZ * 8
    got = pl.pallas_call(
        functools.partial(_attend_kernel, dists=dists, queries=queries, first=first, last=last),
        in_specs=[SMEM] + [VMEM] * (len(args) - 1),
        out_specs=tuple(VMEM for _ in out),
        out_shape=out,
        scratch_shapes=scratch,
        compiler_params=PARAMS,
        cost_estimate=pl.CostEstimate(
            flops=pairs * ROWS * ROWS * HEAD * 4, transcendentals=pairs * ROWS * ROWS, bytes_accessed=4 << 20
        ),
    )(*args)
    return got[0] if last else got


def _combine_kernel(at_ref, flag_ref, own_ref, part_ref, w_ref, att_ref, out_ref):
    x = flag_ref[NX * 32]
    lses = []
    for j in range(NX):
        ext = own_ref[0, :, 8 * HEAD :] if j == 0 else part_ref[(x + j) & 3, :, 8 * HEAD :]
        ext = ext.astype(jnp.float32)
        lses.append(ext[:, 0:8] + ext[:, 8:16] + ext[:, 16:24])
    top = functools.reduce(jnp.maximum, lses)
    ws = [jnp.exp2(v - top) for v in lses]
    total = functools.reduce(jnp.add, ws)
    ws = [w / total for w in ws]
    for h in range(8):
        at = slice(h * HEAD, (h + 1) * HEAD)
        mixed = ws[0][:, h : h + 1] * own_ref[0, :, at].astype(jnp.float32)
        for j in range(1, NX):
            mixed += ws[j][:, h : h + 1] * part_ref[(x + j) & 3, :, at].astype(jnp.float32)
        att_ref[:, at] = mixed.astype(jnp.bfloat16)
    _columns(at_ref, att_ref, w_ref, out_ref, 1)


def _columns(at_ref, att_ref, w_ref, out_ref, flip):
    me = at_ref[0]
    for n in range(2):
        at = pl.multiple_of((me ^ (2 * n + flip)) * 512, 512)
        out_ref[n] = jnp.dot(
            att_ref[...], w_ref[:, pl.ds(at, 512)], preferred_element_type=jnp.float32
        ).astype(out_ref.dtype)


def _keep_kernel(at_ref, att_ref, w_ref, out_ref):
    _columns(at_ref, att_ref, w_ref, out_ref, 0)


def _call(kernel, args, out, flops):
    many = isinstance(out, tuple)
    return pl.pallas_call(
        kernel,
        in_specs=[SMEM if a.dtype == jnp.int32 else VMEM for a in args],
        out_specs=tuple(VMEM for _ in out) if many else VMEM,
        out_shape=out,
        compiler_params=PARAMS,
        cost_estimate=pl.CostEstimate(flops=flops, transcendentals=0, bytes_accessed=5 << 20),
    )(*args)


def _ring(a, dy):
    return _shift(a, dy=dy)


def per_device(queries, keyvalues, stretch_order, block_table, proj_weight):
    kv = keyvalues.reshape(1, 2 * ROWS, 2 * HEAD)
    near = _swap(jnp.broadcast_to(kv, (NZ, 2 * ROWS, 2 * HEAD)), Z_GROUPS)
    q = _swap(jnp.broadcast_to(queries[None], (NX, ROWS, 8 * HEAD)), X_GROUPS)
    flags = _flags(stretch_order, block_table)
    others = (1, 2, 3)
    f1, b1 = _ring(near, 1), _ring(near, -1)
    f2, b2 = _ring(f1, 1), _ring(b1, -1)
    state = _attend(flags, q, [near, f1, b1], (0, 7, 1), None, False, others)
    f3, b3 = _ring(f2, 1), _ring(b2, -1)
    state = _attend(flags, q, [f2, b2], (6, 2), state, False, others)
    f4, b4 = _ring(f3[:2], 1), _ring(b3[2:], -1)
    state = _attend(flags, q, [f3, b3], (5, 3), state, False, others)
    far = jnp.concatenate([f4, b4], axis=0)
    parts = _attend(flags, q, [far], (4,), state, True, others)
    parts = _swap(parts, X_GROUPS)
    chunks = [near, f1, b1, f2, b2, f3, b3, far]
    own = _attend(flags, queries[None], chunks, (0, 7, 1, 6, 2, 5, 3, 4), None, True, (0,))
    me = lax.axis_index("tp").astype(jnp.int32).reshape(1)
    att, give = _call(
        _combine_kernel,
        [me, flags, own, parts, proj_weight],
        (jax.ShapeDtypeStruct((ROWS, 8 * HEAD), jnp.bfloat16), jax.ShapeDtypeStruct((2, ROWS, 512), jnp.bfloat16)),
        2 * ROWS * 1024 * 1024,
    )
    took = lax.ppermute(give, "tp", [(t, t ^ 1) for t in range(4)])
    keep = _call(
        _keep_kernel, [me, att, proj_weight], jax.ShapeDtypeStruct((2, ROWS, 512), jnp.float32), 2 * ROWS * 1024 * 1024
    )
    both = keep + took.astype(jnp.float32)
    beside = lax.ppermute(both[1].astype(jnp.bfloat16), "tp", [(t, t ^ 2) for t in range(4)])
    return (both[0] + beside.astype(jnp.float32)).astype(jnp.bfloat16)


def solution(mesh):
    in_specs = (P("seq", "tp"), P(None, "seq", "tp"), P(), P(), P("tp", None))
    return jax.shard_map(
        per_device, mesh=mesh, in_specs=in_specs, out_specs=P("seq", "tp"), check_vma=False
    )
```

```python
import functools

import jax
import jax.numpy as jnp
from jax import lax
from jax.experimental import pallas as pl
from jax.experimental.pallas import tpu as pltpu
from jax.sharding import PartitionSpec as P


HEAD = 128
ROWS = 128
NX, NZ, NY = 4, 4, 8
SCALE2 = 1.4426950408889634 / HEAD**0.5
NEG = -1e30
KEYS = 4


SMEM = pl.BlockSpec(memory_space=pltpu.SMEM)
VMEM = pl.BlockSpec(memory_space=pltpu.VMEM)
PARAMS = pltpu.CompilerParams(vmem_limit_bytes=26 * 1024 * 1024)


def _shift(a, dx=0, dz=0, dy=0):
    pairs = []
    for x in range(NX):
        for z in range(NZ):
            for y in range(NY):
                src = (x * NZ + z) * NY + y
                dst = (((x + dx) % NX) * NZ + (z + dz) % NZ) * NY + (y + dy) % NY
                pairs.append((src, dst))
    return lax.ppermute(a, "seq", pairs)


X_GROUPS = [[x * NZ * NY + r for x in range(NX)] for r in range(NZ * NY)]
Z_GROUPS = [[(x * NZ + z) * NY + y for z in range(NZ)] for x in range(NX) for y in range(NY)]


def _swap(a, groups):
    return lax.all_to_all(a, "seq", 0, 0, tiled=True, axis_index_groups=groups)


OTHERS = (1, 2, 3)
CALLS = {
    "att1": (OTHERS, (0, 7, 1)),
    "att2": (OTHERS, (6, 2)),
    "att3": (OTHERS, (5, 3)),
    "att4": (OTHERS, (4,)),
    "att_own": ((0,), (0, 7, 1, 6, 2, 5, 3, 4)),
}
PLACES = {}
LIST_END = 2
for _name, (_queries, _dists) in CALLS.items():
    for _j in range(len(_queries)):
        PLACES[_name, _j] = LIST_END
        LIST_END += 1 + len(_dists) * NZ + KEYS


def _lists_kernel(at_ref, order_ref, table_ref, out_ref):
    me = at_ref[0]
    x = lax.shift_right_logical(me, 5)
    z = lax.shift_right_logical(me, 3) & 3
    y = me & 7
    out_ref[0] = x
    out_ref[1] = z
    keys = {(d, n): order_ref[x * 32 + n * 8 + ((y + d) & 7)] for d in range(NY) for n in range(NZ)}
    for name, (queries, dists) in CALLS.items():
        for j, from_x in enumerate(queries):
            mine = order_ref[((x + from_x) & 3) * 32 + z * 8 + y]
            place = PLACES[name, j]
            count = jnp.int32(0)
            for c, d in enumerate(dists):
                for n in range(NZ):
                    key = keys[d, n]
                    out_ref[place + 1 + count] = c * NZ + n
                    count += jnp.where((key < mine) & (table_ref[mine, key] == 1), 1, 0)
            for n in range(KEYS - 1):
                out_ref[place + 1 + count + n] = 0
            out_ref[place] = count


def _lists(order, table):
    me = lax.axis_index("seq").astype(jnp.int32).reshape(1)
    return pl.pallas_call(
        _lists_kernel,
        in_specs=[SMEM, SMEM, SMEM],
        out_specs=SMEM,
        out_shape=jax.ShapeDtypeStruct((LIST_END,), jnp.int32),
        name="lists",
    )(me, order, table)


def _unit(q_ref, i, kv_ref, picks, bias, acc_ref, m_ref, j):
    def rows(part, g):
        return jnp.concatenate(
            [kv_ref[p, part * ROWS : (part + 1) * ROWS, g * HEAD : (g + 1) * HEAD] for p in picks], axis=0
        )

    scores = []
    for g in range(2):
        q = jnp.concatenate([q_ref[i, :, (g * 4 + h) * HEAD : (g * 4 + h + 1) * HEAD] for h in range(4)], axis=0)
        scores.append(
            lax.dot_general(q, rows(0, g), (((1,), (1,)), ((), ())), preferred_element_type=jnp.float32)
        )
    for g in range(2):
        v = rows(1, g)
        v = jnp.concatenate([v, jnp.ones_like(v)], axis=1)
        s = scores[g] * SCALE2 + bias
        heads = slice(g * 4, g * 4 + 4)
        m_old = m_ref[j, heads].reshape(4 * ROWS, HEAD)
        m_new = jnp.maximum(m_old, jnp.max(s, axis=1, keepdims=True))
        p = jnp.exp2(s - jnp.concatenate([m_new] * len(picks), axis=1))
        pv = jnp.dot(p.astype(jnp.bfloat16), v, preferred_element_type=jnp.float32)
        factor = jnp.exp2(m_old - m_new)
        acc = acc_ref[j, heads].reshape(4 * ROWS, 2 * HEAD)
        acc = acc * jnp.concatenate([factor, factor], axis=1) + pv
        acc_ref[j, heads] = acc.reshape(4, ROWS, 2 * HEAD)
        m_ref[j, heads] = m_new.reshape(4, ROWS, HEAD)


def _finish(acc_ref, m_ref, j, out_ref, i):
    col = lax.broadcasted_iota(jnp.int32, (ROWS, HEAD), 1) % 8
    sums = jnp.zeros((ROWS, HEAD), jnp.float32)
    tops = jnp.zeros((ROWS, HEAD), jnp.float32)
    for h in range(8):
        total = acc_ref[j, h, :, HEAD:]
        safe = jnp.where(total > 0.0, total, 1.0)
        out_ref[i, :, h * HEAD : (h + 1) * HEAD] = (acc_ref[j, h, :, :HEAD] / safe).astype(jnp.bfloat16)
        sums = jnp.where(col == h, total, sums)
        tops = jnp.where(col == h, m_ref[j, h], tops)
    some = sums > 0.0
    ext = jnp.where(some, tops + jnp.log2(jnp.where(some, sums, 1.0)), NEG)
    col = lax.broadcasted_iota(jnp.int32, (ROWS, HEAD), 1)
    hi = ext.astype(jnp.bfloat16).astype(jnp.float32)
    left = ext - hi
    mid = left.astype(jnp.bfloat16).astype(jnp.float32)
    ext = jnp.where(col < 8, hi, jnp.where(col < 16, mid, left - mid))
    out_ref[i, :, 8 * HEAD :] = ext.astype(jnp.bfloat16)


def _attend_kernel(*refs, name, first, last):
    queries, dists = CALLS[name]
    nq, nc = len(queries), len(dists)
    own = queries == (0,)
    list_ref, q_ref = refs[:2]
    chunk_refs = refs[2 : 2 + nc]
    rest = list(refs[2 + nc :])
    state = [] if first else [rest.pop(0), rest.pop(0)]
    kv_ref = rest.pop()
    if last:
        out_ref = rest.pop(0)
    acc_ref, m_ref = rest
    for c, ref in enumerate(chunk_refs):
        kv_ref[c * NZ : (c + 1) * NZ] = ref[...]
    if first:
        acc_ref[...] = jnp.zeros_like(acc_ref)
        m_ref[...] = jnp.full_like(m_ref, NEG)
    else:
        acc_ref[...] = state[0][...]
        m_ref[...] = state[1][...]
    if own:
        key = lax.broadcasted_iota(jnp.int32, (ROWS, ROWS), 1)
        row = lax.broadcasted_iota(jnp.int32, (ROWS, ROWS), 0)
        bias = jnp.concatenate([jnp.where(key > row, NEG, 0.0)] * 4, axis=0)
        _unit(q_ref, 0, kv_ref, [list_ref[1]], bias, acc_ref, m_ref, 0)
    lane = lax.broadcasted_iota(jnp.int32, (1, KEYS * ROWS), 1) // ROWS
    x = list_ref[0]
    step = PLACES[name, 1] - PLACES[name, 0] if nq > 1 else 0

    def where_q(j):
        return 0 if own else (x + queries[0] + j) & 3

    def each_query(j, carry):
        place = PLACES[name, 0] + j * step
        count = list_ref[place]

        def each(u, inner):
            picks = [list_ref[place + 1 + u * KEYS + n] for n in range(KEYS)]
            bias = jnp.where(lane + u * KEYS < count, 0.0, NEG)
            _unit(q_ref, where_q(j), kv_ref, picks, bias, acc_ref, m_ref, j)
            return inner

        lax.fori_loop(0, lax.shift_right_logical(count + KEYS - 1, KEYS.bit_length() - 1), each, 0)
        return carry

    if nq == 1:
        each_query(0, 0)
    else:
        lax.fori_loop(0, nq, each_query, 0)
    if last:
        for j in range(nq):
            _finish(acc_ref, m_ref, j, out_ref, where_q(j))


def _attend(name, lists, q, chunks, state, last):
    queries = CALLS[name][0]
    nq, nc = len(queries), len(chunks)
    first = state is None
    args = [lists, q, *chunks] + ([] if first else list(state))
    acc = jax.ShapeDtypeStruct((nq, 8, ROWS, 2 * HEAD), jnp.float32)
    top = jax.ShapeDtypeStruct((nq, 8, ROWS, HEAD), jnp.float32)
    scratch = [pltpu.VMEM((nc * NZ, 2 * ROWS, 2 * HEAD), jnp.bfloat16)]
    if last:
        out = (jax.ShapeDtypeStruct((q.shape[0], ROWS, 9 * HEAD), jnp.bfloat16),)
        scratch = [pltpu.VMEM(acc.shape, acc.dtype), pltpu.VMEM(top.shape, top.dtype)] + scratch
    else:
        out = (acc, top)
    pairs = nq * nc * NZ * 8
    got = pl.pallas_call(
        functools.partial(_attend_kernel, name=name, first=first, last=last),
        in_specs=[SMEM] + [VMEM] * (len(args) - 1),
        out_specs=tuple(VMEM for _ in out),
        out_shape=out,
        scratch_shapes=scratch,
        compiler_params=PARAMS,
        cost_estimate=pl.CostEstimate(
            flops=pairs * ROWS * ROWS * HEAD * 4, transcendentals=pairs * ROWS * ROWS, bytes_accessed=4 << 20
        ),
    )(*args)
    return got[0] if last else got


def _combine_kernel(at_ref, list_ref, own_ref, part_ref, w_ref, att_ref, out_ref):
    x = list_ref[0]
    lses = []
    for j in range(NX):
        ext = own_ref[0, :, 8 * HEAD :] if j == 0 else part_ref[(x + j) & 3, :, 8 * HEAD :]
        ext = ext.astype(jnp.float32)
        lses.append(ext[:, 0:8] + ext[:, 8:16] + ext[:, 16:24])
    top = functools.reduce(jnp.maximum, lses)
    ws = [jnp.exp2(v - top) for v in lses]
    total = functools.reduce(jnp.add, ws)
    ws = [w / total for w in ws]
    for h in range(8):
        at = slice(h * HEAD, (h + 1) * HEAD)
        mixed = ws[0][:, h : h + 1] * own_ref[0, :, at].astype(jnp.float32)
        for j in range(1, NX):
            mixed += ws[j][:, h : h + 1] * part_ref[(x + j) & 3, :, at].astype(jnp.float32)
        att_ref[:, at] = mixed.astype(jnp.bfloat16)
    _columns(at_ref, att_ref, w_ref, out_ref, 1)


def _columns(at_ref, att_ref, w_ref, out_ref, flip):
    me = at_ref[0]
    for n in range(2):
        at = pl.multiple_of((me ^ (2 * n + flip)) * 512, 512)
        out_ref[n] = jnp.dot(
            att_ref[...], w_ref[:, pl.ds(at, 512)], preferred_element_type=jnp.float32
        ).astype(out_ref.dtype)


def _keep_kernel(at_ref, att_ref, w_ref, out_ref):
    _columns(at_ref, att_ref, w_ref, out_ref, 0)


def _call(kernel, args, out, flops):
    many = isinstance(out, tuple)
    return pl.pallas_call(
        kernel,
        in_specs=[SMEM if a.dtype == jnp.int32 else VMEM for a in args],
        out_specs=tuple(VMEM for _ in out) if many else VMEM,
        out_shape=out,
        compiler_params=PARAMS,
        cost_estimate=pl.CostEstimate(flops=flops, transcendentals=0, bytes_accessed=5 << 20),
    )(*args)


def _ring(a, dy):
    return _shift(a, dy=dy)


def per_device(queries, keyvalues, stretch_order, block_table, proj_weight):
    kv = keyvalues.reshape(1, 2 * ROWS, 2 * HEAD)
    near = lax.all_gather(kv, "seq", axis=0, tiled=True, axis_index_groups=Z_GROUPS)
    q = _swap(jnp.broadcast_to(queries[None], (NX, ROWS, 8 * HEAD)), X_GROUPS)
    lists = _lists(stretch_order, block_table)
    f1, b1 = _ring(near, 1), _ring(near, -1)
    f2, b2 = _ring(f1, 1), _ring(b1, -1)
    state = _attend("att1", lists, q, [near, f1, b1], None, False)
    f3, b3 = _ring(f2, 1), _ring(b2, -1)
    state = _attend("att2", lists, q, [f2, b2], state, False)
    f4, b4 = _ring(f3[:2], 1), _ring(b3[2:], -1)
    state = _attend("att3", lists, q, [f3, b3], state, False)
    far = jnp.concatenate([f4, b4], axis=0)
    parts = _attend("att4", lists, q, [far], state, True)
    parts = _swap(parts, X_GROUPS)
    chunks = [near, f1, b1, f2, b2, f3, b3, far]
    own = _attend("att_own", lists, queries[None], chunks, None, True)
    me = lax.axis_index("tp").astype(jnp.int32).reshape(1)
    att, give = _call(
        _combine_kernel,
        [me, lists, own, parts, proj_weight],
        (jax.ShapeDtypeStruct((ROWS, 8 * HEAD), jnp.bfloat16), jax.ShapeDtypeStruct((2, ROWS, 512), jnp.bfloat16)),
        2 * ROWS * 1024 * 1024,
    )
    took = lax.ppermute(give, "tp", [(t, t ^ 1) for t in range(4)])
    keep = _call(
        _keep_kernel,
        [me, att, proj_weight],
        jax.ShapeDtypeStruct((2, ROWS, 512), jnp.float32),
        2 * ROWS * 1024 * 1024,
    )
    both = keep + took.astype(jnp.float32)
    beside = lax.ppermute(both[1].astype(jnp.bfloat16), "tp", [(t, t ^ 2) for t in range(4)])
    return (both[0] + beside.astype(jnp.float32)).astype(jnp.bfloat16)


def solution(mesh):
    in_specs = (P("seq", "tp"), P(None, "seq", "tp"), P(), P(), P("tp", None))
    return jax.shard_map(
        per_device, mesh=mesh, in_specs=in_specs, out_specs=P("seq", "tp"), check_vma=False
    )
```

```python
import functools

import jax
import jax.numpy as jnp
from jax import lax
from jax.experimental import pallas as pl
from jax.experimental.pallas import tpu as pltpu
from jax.sharding import PartitionSpec as P


HEAD = 128
ROWS = 128
NX, NZ, NY = 4, 4, 8
SCALE2 = 1.4426950408889634 / HEAD**0.5
NEG = -1e30
KEYS = 4


SMEM = pl.BlockSpec(memory_space=pltpu.SMEM)
VMEM = pl.BlockSpec(memory_space=pltpu.VMEM)
PARAMS = pltpu.CompilerParams(vmem_limit_bytes=26 * 1024 * 1024)


def _shift(a, dx=0, dz=0, dy=0):
    pairs = []
    for x in range(NX):
        for z in range(NZ):
            for y in range(NY):
                src = (x * NZ + z) * NY + y
                dst = (((x + dx) % NX) * NZ + (z + dz) % NZ) * NY + (y + dy) % NY
                pairs.append((src, dst))
    return lax.ppermute(a, "seq", pairs)


X_GROUPS = [[x * NZ * NY + r for x in range(NX)] for r in range(NZ * NY)]
Z_GROUPS = [[(x * NZ + z) * NY + y for z in range(NZ)] for x in range(NX) for y in range(NY)]


def _swap(a, groups):
    return lax.all_to_all(a, "seq", 0, 0, tiled=True, axis_index_groups=groups)


OTHERS = (1, 2, 3)
CALLS = {
    "att1": (OTHERS, (0, 7, 1)),
    "att2": (OTHERS, (6, 2)),
    "att3": (OTHERS, (5, 3)),
    "att4": (OTHERS, (4,)),
    "own1": ((0,), (0, 7, 1)),
    "own2": ((0,), (6, 2, 5, 3, 4)),
}
PLACES = {}
LIST_END = 2
for _name, (_queries, _dists) in CALLS.items():
    for _j in range(len(_queries)):
        PLACES[_name, _j] = LIST_END
        LIST_END += 1 + len(_dists) * NZ + KEYS


def _lists_kernel(at_ref, order_ref, table_ref, out_ref):
    me = at_ref[0]
    x = lax.shift_right_logical(me, 5)
    z = lax.shift_right_logical(me, 3) & 3
    y = me & 7
    out_ref[0] = x
    out_ref[1] = z
    keys = {(d, n): order_ref[x * 32 + n * 8 + ((y + d) & 7)] for d in range(NY) for n in range(NZ)}
    for from_x in range(NX):
        mine = order_ref[((x + from_x) & 3) * 32 + z * 8 + y]
        seen = {
            at: jnp.where((key < mine) & (table_ref[mine, key] == 1), 1, 0) for at, key in keys.items()
        }
        for name, (queries, dists) in CALLS.items():
            if from_x not in queries:
                continue
            place = PLACES[name, queries.index(from_x)]
            count = jnp.int32(0)
            for c, d in enumerate(dists):
                for n in range(NZ):
                    out_ref[place + 1 + count] = c * NZ + n
                    count += seen[d, n]
            for n in range(KEYS - 1):
                out_ref[place + 1 + count + n] = 0
            out_ref[place] = count


def _lists(order, table):
    me = lax.axis_index("seq").astype(jnp.int32).reshape(1)
    return pl.pallas_call(
        _lists_kernel,
        in_specs=[SMEM, SMEM, SMEM],
        out_specs=SMEM,
        out_shape=jax.ShapeDtypeStruct((LIST_END,), jnp.int32),
        name="lists",
    )(me, order, table)


def _unit(q_ref, i, kv_ref, picks, bias, acc_ref, m_ref, j):
    def rows(part, g):
        return jnp.concatenate(
            [kv_ref[p, part * ROWS : (part + 1) * ROWS, g * HEAD : (g + 1) * HEAD] for p in picks], axis=0
        )

    scores = []
    for g in range(2):
        q = jnp.concatenate([q_ref[i, :, (g * 4 + h) * HEAD : (g * 4 + h + 1) * HEAD] for h in range(4)], axis=0)
        scores.append(
            lax.dot_general(q, rows(0, g), (((1,), (1,)), ((), ())), preferred_element_type=jnp.float32)
        )
    for g in range(2):
        v = rows(1, g)
        v = jnp.concatenate([v, jnp.ones_like(v)], axis=1)
        s = scores[g] * SCALE2 + bias
        heads = slice(g * 4, g * 4 + 4)
        m_old = m_ref[j, heads].reshape(4 * ROWS, HEAD)
        m_new = jnp.maximum(m_old, jnp.max(s, axis=1, keepdims=True))
        p = jnp.exp2(s - jnp.concatenate([m_new] * len(picks), axis=1))
        pv = jnp.dot(p.astype(jnp.bfloat16), v, preferred_element_type=jnp.float32)
        factor = jnp.exp2(m_old - m_new)
        acc = acc_ref[j, heads].reshape(4 * ROWS, 2 * HEAD)
        acc = acc * jnp.concatenate([factor, factor], axis=1) + pv
        acc_ref[j, heads] = acc.reshape(4, ROWS, 2 * HEAD)
        m_ref[j, heads] = m_new.reshape(4, ROWS, HEAD)


def _finish(acc_ref, m_ref, j, out_ref, i):
    col = lax.broadcasted_iota(jnp.int32, (ROWS, HEAD), 1) % 8
    sums = jnp.zeros((ROWS, HEAD), jnp.float32)
    tops = jnp.zeros((ROWS, HEAD), jnp.float32)
    for h in range(8):
        total = acc_ref[j, h, :, HEAD:]
        safe = jnp.where(total > 0.0, total, 1.0)
        out_ref[i, :, h * HEAD : (h + 1) * HEAD] = (acc_ref[j, h, :, :HEAD] / safe).astype(jnp.bfloat16)
        sums = jnp.where(col == h, total, sums)
        tops = jnp.where(col == h, m_ref[j, h], tops)
    some = sums > 0.0
    ext = jnp.where(some, tops + jnp.log2(jnp.where(some, sums, 1.0)), NEG)
    col = lax.broadcasted_iota(jnp.int32, (ROWS, HEAD), 1)
    hi = ext.astype(jnp.bfloat16).astype(jnp.float32)
    left = ext - hi
    mid = left.astype(jnp.bfloat16).astype(jnp.float32)
    ext = jnp.where(col < 8, hi, jnp.where(col < 16, mid, left - mid))
    out_ref[i, :, 8 * HEAD :] = ext.astype(jnp.bfloat16)


def _attend_kernel(*refs, name, first, last):
    queries, dists = CALLS[name]
    nq, nc = len(queries), len(dists)
    own = queries == (0,)
    list_ref, q_ref = refs[:2]
    chunk_refs = refs[2 : 2 + nc]
    rest = list(refs[2 + nc :])
    state = [] if first else [rest.pop(0), rest.pop(0)]
    kv_ref = rest.pop()
    if last:
        out_ref = rest.pop(0)
    acc_ref, m_ref = rest
    for c, ref in enumerate(chunk_refs):
        kv_ref[c * NZ : (c + 1) * NZ] = ref[...]
    if first:
        acc_ref[...] = jnp.zeros_like(acc_ref)
        m_ref[...] = jnp.full_like(m_ref, NEG)
    else:
        acc_ref[...] = state[0][...]
        m_ref[...] = state[1][...]
    if own and dists[0] == 0:
        key = lax.broadcasted_iota(jnp.int32, (ROWS, ROWS), 1)
        row = lax.broadcasted_iota(jnp.int32, (ROWS, ROWS), 0)
        bias = jnp.concatenate([jnp.where(key > row, NEG, 0.0)] * 4, axis=0)
        _unit(q_ref, 0, kv_ref, [list_ref[1]], bias, acc_ref, m_ref, 0)
    lane = lax.broadcasted_iota(jnp.int32, (1, KEYS * ROWS), 1) // ROWS
    x = list_ref[0]
    step = PLACES[name, 1] - PLACES[name, 0] if nq > 1 else 0

    def where_q(j):
        return 0 if own else (x + queries[0] + j) & 3

    def each_query(j, carry):
        place = PLACES[name, 0] + j * step
        count = list_ref[place]

        def each(u, inner):
            picks = [list_ref[place + 1 + u * KEYS + n] for n in range(KEYS)]
            bias = jnp.where(lane + u * KEYS < count, 0.0, NEG)
            _unit(q_ref, where_q(j), kv_ref, picks, bias, acc_ref, m_ref, j)
            return inner

        lax.fori_loop(0, lax.shift_right_logical(count + KEYS - 1, KEYS.bit_length() - 1), each, 0)
        return carry

    if nq == 1:
        each_query(0, 0)
    else:
        lax.fori_loop(0, nq, each_query, 0)
    if last:
        for j in range(nq):
            _finish(acc_ref, m_ref, j, out_ref, where_q(j))


def _attend(name, lists, q, chunks, state, last):
    queries = CALLS[name][0]
    nq, nc = len(queries), len(chunks)
    first = state is None
    args = [lists, q, *chunks] + ([] if first else list(state))
    acc = jax.ShapeDtypeStruct((nq, 8, ROWS, 2 * HEAD), jnp.float32)
    top = jax.ShapeDtypeStruct((nq, 8, ROWS, HEAD), jnp.float32)
    scratch = [pltpu.VMEM((nc * NZ, 2 * ROWS, 2 * HEAD), jnp.bfloat16)]
    if last:
        out = (jax.ShapeDtypeStruct((q.shape[0], ROWS, 9 * HEAD), jnp.bfloat16),)
        scratch = [pltpu.VMEM(acc.shape, acc.dtype), pltpu.VMEM(top.shape, top.dtype)] + scratch
    else:
        out = (acc, top)
    pairs = nq * nc * NZ * 8
    got = pl.pallas_call(
        functools.partial(_attend_kernel, name=name, first=first, last=last),
        in_specs=[SMEM] + [VMEM] * (len(args) - 1),
        out_specs=tuple(VMEM for _ in out),
        out_shape=out,
        scratch_shapes=scratch,
        compiler_params=PARAMS,
        cost_estimate=pl.CostEstimate(
            flops=pairs * ROWS * ROWS * HEAD * 4, transcendentals=pairs * ROWS * ROWS, bytes_accessed=4 << 20
        ),
    )(*args)
    return got[0] if last else got


def _combine_kernel(at_ref, list_ref, own1_ref, own2_ref, part_ref, w_ref, att_ref, out_ref):
    x = list_ref[0]
    sources = [(own1_ref, 0), (own2_ref, 0)] + [(part_ref, (x + j) & 3) for j in range(1, NX)]
    lses = []
    for ref, i in sources:
        ext = ref[i, :, 8 * HEAD :].astype(jnp.float32)
        lses.append(ext[:, 0:8] + ext[:, 8:16] + ext[:, 16:24])
    top = functools.reduce(jnp.maximum, lses)
    ws = [jnp.exp2(v - top) for v in lses]
    total = functools.reduce(jnp.add, ws)
    ws = [w / total for w in ws]
    for h in range(8):
        at = slice(h * HEAD, (h + 1) * HEAD)
        mixed = jnp.zeros((ROWS, HEAD), jnp.float32)
        for w, (ref, i) in zip(ws, sources):
            mixed += w[:, h : h + 1] * ref[i, :, at].astype(jnp.float32)
        att_ref[:, at] = mixed.astype(jnp.bfloat16)
    _columns(at_ref, att_ref, w_ref, out_ref, 1)


def _columns(at_ref, att_ref, w_ref, out_ref, flip):
    me = at_ref[0]
    for n in range(2):
        at = pl.multiple_of((me ^ (2 * n + flip)) * 512, 512)
        out_ref[n] = jnp.dot(
            att_ref[...], w_ref[:, pl.ds(at, 512)], preferred_element_type=jnp.float32
        ).astype(out_ref.dtype)


def _keep_kernel(at_ref, att_ref, w_ref, out_ref):
    _columns(at_ref, att_ref, w_ref, out_ref, 0)


def _call(kernel, args, out, flops):
    many = isinstance(out, tuple)
    return pl.pallas_call(
        kernel,
        in_specs=[SMEM if a.dtype == jnp.int32 else VMEM for a in args],
        out_specs=tuple(VMEM for _ in out) if many else VMEM,
        out_shape=out,
        compiler_params=PARAMS,
        cost_estimate=pl.CostEstimate(flops=flops, transcendentals=0, bytes_accessed=5 << 20),
    )(*args)


def _ring(a, dy):
    return _shift(a, dy=dy)


def per_device(queries, keyvalues, stretch_order, block_table, proj_weight):
    kv = keyvalues.reshape(1, 2 * ROWS, 2 * HEAD)
    near = lax.all_gather(kv, "seq", axis=0, tiled=True, axis_index_groups=Z_GROUPS)
    q = _swap(jnp.broadcast_to(queries[None], (NX, ROWS, 8 * HEAD)), X_GROUPS)
    lists = _lists(stretch_order, block_table)
    f1, b1 = _ring(near, 1), _ring(near, -1)
    f2, b2 = _ring(f1, 1), _ring(b1, -1)
    state = _attend("att1", lists, q, [near, f1, b1], None, False)
    own1 = _attend("own1", lists, queries[None], [near, f1, b1], None, True)
    f3, b3 = _ring(f2, 1), _ring(b2, -1)
    state = _attend("att2", lists, q, [f2, b2], state, False)
    f4, b4 = _ring(f3[:2], 1), _ring(b3[2:], -1)
    state = _attend("att3", lists, q, [f3, b3], state, False)
    far = jnp.concatenate([f4, b4], axis=0)
    parts = _attend("att4", lists, q, [far], state, True)
    parts = _swap(parts, X_GROUPS)
    own2 = _attend("own2", lists, queries[None], [f2, b2, f3, b3, far], None, True)
    me = lax.axis_index("tp").astype(jnp.int32).reshape(1)
    att, give = _call(
        _combine_kernel,
        [me, lists, own1, own2, parts, proj_weight],
        (jax.ShapeDtypeStruct((ROWS, 8 * HEAD), jnp.bfloat16), jax.ShapeDtypeStruct((2, ROWS, 512), jnp.bfloat16)),
        2 * ROWS * 1024 * 1024,
    )
    took = lax.ppermute(give, "tp", [(t, t ^ 1) for t in range(4)])
    keep = _call(
        _keep_kernel, [me, att, proj_weight], jax.ShapeDtypeStruct((2, ROWS, 512), jnp.float32), 2 * ROWS * 1024 * 1024
    )
    both = keep + took.astype(jnp.float32)
    beside = lax.ppermute(both[1].astype(jnp.bfloat16), "tp", [(t, t ^ 2) for t in range(4)])
    return (both[0] + beside.astype(jnp.float32)).astype(jnp.bfloat16)


def solution(mesh):
    in_specs = (P("seq", "tp"), P(None, "seq", "tp"), P(), P(), P("tp", None))
    return jax.shard_map(
        per_device, mesh=mesh, in_specs=in_specs, out_specs=P("seq", "tp"), check_vma=False
    )
```
